128 devices in a mesh: utt: 8 (over y, core), clu: 16 (over z, x).
Axes of the slice: x: 4, y: 4, z: 4, core: 2. Of those that a mesh axis runs over, the one named last changes fastest.
Arguments:
- features: bfloat16 [262144, 1280], P(('utt', 'clu')), may hold values from -1.75 to 1.75
- centroids: bfloat16 [2048, 1280], P('clu'), may hold values from -2 to 2
- route: int32 [128, 128], P(('utt', 'clu')), may hold values from 0 to 127, each once within a row
Outputs:
- trainer_labels: int32 [128, 128, 16], P(('utt', 'clu'))
- trainer_distance: float32 [128, 128, 16], P(('utt', 'clu'))
The draws below stay inside these ranges and needn't reach their ends.
Inputs may be any that keep to these rules, and one draw needn't show every extreme that they name: Each row of route names every trainer device exactly once.
All inputs are finite; a program needn't handle non-finite values.
Results may differ from the reference program's by a relative error of at most 0.0003.
Values may be sent and summed in bfloat16 or wider, within the bound.
No kernel may reach another device: no remote copies, remote signals or barrier semaphores. Data moves between devices by JAX's collectives and lax.ppermute only.
A program may use at most 64 MiB of HBM per device.

```python
import jax
import jax.numpy as jnp
from jax import lax

D = 1280
K = 2048
FRAMES = 262144
DEVICES = 128


def joint_draw(key):
    base = jax.random.fold_in(key, 7)
    k_cent, k_pick, k_mask, k_noise = jax.random.split(base, 4)
    cent_int = jax.random.randint(k_cent, (K, D), -128, 129)
    noise = jax.random.randint(k_noise, (FRAMES, D), -10, 11)
    keep = jax.random.randint(k_mask, (FRAMES, D), 0, 4) == 0
    picks = jax.random.randint(k_pick, (FRAMES,), 0, K)
    signal = jnp.where(keep, cent_int[picks] // 32, 0)
    feat_int = signal + noise
    feats = feat_int.astype(jnp.float32) / 8.0
    cent = cent_int.astype(jnp.float32) / 64.0
    return (feats, cent)


def draw_features(key, part):
    return joint_draw(key)[0].astype(jnp.bfloat16)


def draw_centroids(key, part):
    return joint_draw(key)[1].astype(jnp.bfloat16)


def setup_inputs(seed: int = 0) -> dict:
    arg_keys = jax.random.split(jax.random.key(seed), 4)
    features = draw_features(jax.random.fold_in(arg_keys[3], 71), 0)
    centroids = draw_centroids(jax.random.fold_in(arg_keys[3], 71), 0)
    route = jax.vmap(lambda own: jax.random.permutation(own, DEVICES))(jax.random.split(arg_keys[2], DEVICES)).reshape((DEVICES, DEVICES)).astype(jnp.int32)
    return {"features": features, "centroids": centroids, "route": route}


def reference(features, centroids, route):
    cent_sq = jnp.sum(jnp.square(centroids.astype(jnp.float32)), axis=1)
    step = 1024
    blocks = features.reshape(FRAMES // step, step, D)

    def nearest(block):
        frame_sq = jnp.sum(jnp.square(block.astype(jnp.float32)), axis=1)
        inner = jnp.dot(block, centroids.T, preferred_element_type=jnp.float32)
        dist = (frame_sq[:, None] - 2.0 * inner + cent_sq[None, :]) / D
        return jnp.argmin(dist, axis=1).astype(jnp.int32), jnp.min(dist, axis=1)

    labels, least = lax.map(nearest, blocks)
    devices = route.shape[0]
    labels = labels.reshape(devices, devices, FRAMES // (devices * devices))
    least = least.reshape(devices, devices, FRAMES // (devices * devices))
    inverse = jnp.argsort(route, axis=1).astype(jnp.int32)
    picked_labels = jnp.take_along_axis(labels, inverse[:, :, None], axis=1)
    picked_least = jnp.take_along_axis(least, inverse[:, :, None], axis=1)
    return jnp.transpose(picked_labels, (1, 0, 2)), jnp.transpose(picked_least, (1, 0, 2))
```

```python
import functools

import jax
import jax.numpy as jnp
from jax import lax
from jax.experimental import pallas as pl
from jax.experimental.pallas import tpu as pltpu
from jax.sharding import PartitionSpec as P


AXES = ("utt", "clu")
SIDE = 4
OFFSETS = (0, 1, -1, 2)
VMEM = pltpu.VMEM
F32 = jnp.float32
BF16 = jnp.bfloat16
BIG = 1 << 20


def device(y, c, z, x):
    return (y * 2 + c) * 16 + (z % SIDE) * SIDE + x % SIDE


def along(offset, phase):
    pairs = []
    for y in range(4):
        for c in range(2):
            for z in range(SIDE):
                for x in range(SIDE):
                    on_x = (c == 0) == (phase == 0)
                    target = device(y, c, z, x + offset) if on_x else device(y, c, z + offset, x)
                    pairs.append((device(y, c, z, x), target))
    return pairs


def core_swap():
    return [
        (device(y, c, z, x), device(y, 1 - c, z, x))
        for y in range(4)
        for c in range(2)
        for z in range(SIDE)
        for x in range(SIDE)
    ]


def block_base(chunk, block, rows):
    core = lax.rem(lax.axis_index("utt"), 2)
    clu = lax.axis_index("clu")
    z, x = clu // SIDE, lax.rem(clu, SIDE)
    far = (SIDE - OFFSETS[chunk]) % SIDE
    near = (SIDE - OFFSETS[block]) % SIDE
    from_z = lax.rem(z + jnp.where(core == 0, far, near), SIDE)
    from_x = lax.rem(x + jnp.where(core == 0, near, far), SIDE)
    return (from_z * SIDE + from_x) * (2 * rows) + core * rows


def transpose_kernel(feat_ref, out_ref, sq_ref):
    frames, width = feat_ref.shape
    cell = 256
    eye = (
        lax.broadcasted_iota(jnp.int32, (cell, cell), 0) == lax.broadcasted_iota(jnp.int32, (cell, cell), 1)
    ).astype(BF16)
    for f in range(0, frames, 512):
        total = jnp.zeros((8, 512), F32)
        for k in range(0, width, cell):
            part = lax.dot_general(
                eye, feat_ref[f : f + 512, k : k + cell], (((1,), (1,)), ((), ())), preferred_element_type=F32
            )
            out_ref[k : k + cell, f : f + 512] = part.astype(BF16)
            total = total + jnp.sum((part * part).reshape(cell // 8, 8, 512), axis=0)
        sq_ref[:, f : f + 512] = jnp.broadcast_to(jnp.sum(total, axis=0, keepdims=True), (8, 512))


def transposed(features):
    frames, width = features.shape
    return pl.pallas_call(
        transpose_kernel,
        out_shape=(jax.ShapeDtypeStruct((width, frames), BF16), jax.ShapeDtypeStruct((8, frames), F32)),
        in_specs=[pl.BlockSpec(memory_space=VMEM)],
        out_specs=(pl.BlockSpec(memory_space=VMEM),) * 2,
        compiler_params=pltpu.CompilerParams(vmem_limit_bytes=14 << 20),
        cost_estimate=pl.CostEstimate(flops=8 << 30, bytes_accessed=10 << 20, transcendentals=0),
        name="transposed",
    )(features)


def score(chunk, cents_ref, own_ref, other_ref, least_in, index_in, least_ref, index_ref):
    rows = cents_ref.shape[0] // len(OFFSETS)
    frames = own_ref.shape[1]
    tile = 512
    cents = cents_ref[...]
    wide = cents.astype(F32)
    cent_sq = jnp.sum(wide * wide, axis=1, keepdims=True)
    scaled = cents * BF16(-2)
    sub = lax.broadcasted_iota(jnp.int32, (8, tile), 0)
    for side, feats in enumerate((own_ref, other_ref)):
        for f in range(0, frames, tile):
            at = slice(side * frames + f, side * frames + f + tile)
            dots = jnp.dot(scaled, feats[:, f : f + tile], preferred_element_type=F32)
            least = index = None
            if least_in is not None:
                least, index = least_in[:, at], index_in[:, at]
            for block in range(len(OFFSETS)):
                low = where = None
                for r in range(0, rows, 8):
                    q = block * rows + r
                    value = dots[q : q + 8] + cent_sq[q : q + 8]
                    if low is None:
                        low, where = value, jnp.zeros((8, tile), jnp.int32)
                    else:
                        less = value < low
                        low = jnp.where(less, value, low)
                        where = jnp.where(less, r, where)
                where = where + (sub + block_base(chunk, block, rows))
                if least is None:
                    least, index = low, where
                else:
                    better = (low < least) | ((low == least) & (where < index))
                    least = jnp.where(better, low, least)
                    index = jnp.where(better, where, index)
            least_ref[:, at] = least
            index_ref[:, at] = index


def pieces(value):
    high = value.astype(BF16)
    rest = value - high.astype(F32)
    middle = rest.astype(BF16)
    low = (rest - middle.astype(F32)).astype(BF16)
    return high, middle, low


def exact_dot(left, right):
    if left.dtype == F32:
        parts = [jnp.dot(p, right, preferred_element_type=F32) for p in pieces(left)]
    else:
        parts = [jnp.dot(left, p, preferred_element_type=F32) for p in pieces(right)]
    return (parts[0] + parts[1]) + parts[2]


def pack(least, index, square_ref, route_ref, other_route_ref, out_ref):
    frames = least.shape[1] // 2
    low = jnp.min(least, axis=0, keepdims=True)
    label = jnp.min(jnp.where(least == low, index, BIG), axis=0, keepdims=True).astype(F32)
    square = square_ref[0:1, :]
    sub = lax.broadcasted_iota(jnp.int32, (8, 128), 0)
    lane = lax.broadcasted_iota(jnp.int32, (8, 128), 1)
    mask = (lane // 16) == sub
    src = lax.broadcasted_iota(jnp.int32, (128, 128), 0)
    dst = lax.broadcasted_iota(jnp.int32, (128, 128), 1)

    def spread(row):
        groups = [
            jnp.where(mask, jnp.broadcast_to(row[:, i : i + 128], (8, 128)), 0.0) for i in range(0, frames, 128)
        ]
        return jnp.concatenate(groups, axis=0)

    def place(row, slot):
        pick = (dst == slot * 16 + lax.rem(src, 16)).astype(BF16)
        return exact_dot(spread(row), pick)

    own = place(low[:, :frames], 0) + place(label[:, :frames], 1) + place(square, 4)
    other = place(low[:, frames:], 2) + place(label[:, frames:], 3)
    to_own = (src == route_ref[0:1, :]).astype(BF16)
    to_other = (src == other_route_ref[0:1, :]).astype(BF16)
    out_ref[...] = exact_dot(to_own, own) + exact_dot(to_other, other)


def first_kernel(cents, own, other, least_ref, index_ref):
    score(0, cents, own, other, None, None, least_ref, index_ref)


def next_kernel(chunk, cents, own, other, least_in, index_in, least_ref, index_ref):
    score(chunk, cents, own, other, least_in, index_in, least_ref, index_ref)


def last_kernel(
    chunk, cents, own, other, least_in, index_in, square, route, other_route, out_ref, least_ref, index_ref
):
    score(chunk, cents, own, other, least_in, index_in, least_ref, index_ref)
    pack(least_ref[...], index_ref[...], square, route, other_route, out_ref)


def scoring(kernel, args, out_shape, scratch=(), name=None):
    return pl.pallas_call(
        kernel,
        out_shape=out_shape,
        in_specs=[pl.BlockSpec(memory_space=VMEM)] * len(args),
        out_specs=jax.tree.map(lambda _: pl.BlockSpec(memory_space=VMEM), out_shape),
        scratch_shapes=list(scratch),
        compiler_params=pltpu.CompilerParams(vmem_limit_bytes=20 << 20),
        cost_estimate=pl.CostEstimate(flops=2 * 256 * 1280 * 4096, bytes_accessed=11 << 20, transcendentals=0),
        name=name,
    )(*args)


def merge_kernel(got_ref, label_ref, dist_ref, *, width):
    got = got_ref[...]
    turned = jnp.concatenate([got[r ^ 16 : (r ^ 16) + 16] for r in range(0, got.shape[0], 16)], axis=0)
    mine, theirs = got.T, turned.T
    low, label = mine[0:16], mine[16:32]
    other_low, other_label = theirs[32:48], theirs[48:64]
    better = (other_low < low) | ((other_low == low) & (other_label < label))
    label_ref[...] = jnp.where(better, other_label, label).astype(jnp.int32)
    dist_ref[...] = (mine[64:80] + jnp.where(better, other_low, low)) / width


def per_device(features, centroids, route):
    frames, width = features.shape
    half = centroids.shape[0] // 2
    core = lax.rem(lax.axis_index("utt"), 2)
    mine = lax.dynamic_slice_in_dim(centroids, core * half, half, axis=0)
    near = [mine] + [lax.ppermute(mine, AXES, along(o, 0)) for o in OFFSETS[1:]]
    own, square = transposed(features)
    other = lax.ppermute(own, AXES, core_swap())
    other_route = lax.ppermute(route, AXES, core_swap())
    chunk0 = jnp.concatenate(near, axis=0)
    far = [lax.ppermute(chunk0, AXES, along(o, 1)) for o in OFFSETS[1:]]
    state = (jax.ShapeDtypeStruct((8, 2 * frames), F32), jax.ShapeDtypeStruct((8, 2 * frames), jnp.int32))
    least, index = scoring(first_kernel, (chunk0, own, other), state, name="score_0")
    for i in (1, 2):
        least, index = scoring(
            functools.partial(next_kernel, i), (far[i - 1], own, other, least, index), state, name=f"score_{i}"
        )
    packed = scoring(
        functools.partial(last_kernel, 3),
        (far[2], own, other, least, index, square, route, other_route),
        jax.ShapeDtypeStruct((128, 128), F32),
        scratch=[pltpu.VMEM((8, 2 * frames), F32), pltpu.VMEM((8, 2 * frames), jnp.int32)],
        name="score_3",
    )
    got = lax.all_to_all(packed, AXES, split_axis=0, concat_axis=0, tiled=True)
    label, dist = pl.pallas_call(
        functools.partial(merge_kernel, width=float(width)),
        out_shape=(jax.ShapeDtypeStruct((16, 128), jnp.int32), jax.ShapeDtypeStruct((16, 128), F32)),
        in_specs=[pl.BlockSpec(memory_space=VMEM)],
        out_specs=(pl.BlockSpec(memory_space=VMEM),) * 2,
        name="merge",
    )(got)
    return label.T[None], dist.T[None]


def solution(mesh):
    placed = (P(AXES, None), P("clu", None), P(AXES, None))
    return jax.shard_map(
        per_device,
        mesh=mesh,
        in_specs=placed,
        out_specs=(P(AXES, None, None), P(AXES, None, None)),
        check_vma=False,
    )
```

```python
import functools

import jax
import jax.numpy as jnp
from jax import lax
from jax.experimental import pallas as pl
from jax.experimental.pallas import tpu as pltpu
from jax.sharding import PartitionSpec as P


AXES = ("utt", "clu")
SIDE = 4
OFFSETS = (0, 1, -1, 2)
VMEM = pltpu.VMEM
F32 = jnp.float32
BF16 = jnp.bfloat16
BIG = 1 << 20


def device(y, c, z, x):
    return (y * 2 + c) * 16 + (z % SIDE) * SIDE + x % SIDE


def along(offset, phase):
    pairs = []
    for y in range(4):
        for c in range(2):
            for z in range(SIDE):
                for x in range(SIDE):
                    on_x = (c == 0) == (phase == 0)
                    target = device(y, c, z, x + offset) if on_x else device(y, c, z + offset, x)
                    pairs.append((device(y, c, z, x), target))
    return pairs


def core_swap():
    return [
        (device(y, c, z, x), device(y, 1 - c, z, x))
        for y in range(4)
        for c in range(2)
        for z in range(SIDE)
        for x in range(SIDE)
    ]


def fetch(step):
    pairs = []
    for y in range(4):
        for c in range(2):
            for z in range(SIDE):
                for x in range(SIDE):
                    near = y % 2 + 2 * step
                    target = device(y, c, z - 2, x - near) if c == 0 else device(y, c, z - near, x - 2)
                    pairs.append((device(y, c, z, x), target))
    return pairs


def plane_swap():
    return [
        (device(y, c, z, x), device(y ^ 1, c, z, x))
        for y in range(4)
        for c in range(2)
        for z in range(SIDE)
        for x in range(SIDE)
    ]


def block_base(far, near, rows):
    core = lax.rem(lax.axis_index("utt"), 2)
    clu = lax.axis_index("clu")
    z, x = clu // SIDE, lax.rem(clu, SIDE)
    from_z = lax.rem(z + jnp.where(core == 0, far, near), SIDE)
    from_x = lax.rem(x + jnp.where(core == 0, near, far), SIDE)
    return (from_z * SIDE + from_x) * (2 * rows) + core * rows


def row_bases(far, rows):
    return [block_base((SIDE - far) % SIDE, (SIDE - near) % SIDE, rows) for near in OFFSETS]


def pair_bases(own, rows):
    plane = lax.rem(lax.axis_index("utt") // 2, 2)
    first = plane if own else 1 - plane
    return [block_base(2, lax.rem(first + 2 * step, SIDE), rows) for step in range(2)]


def cut_kernel(cents_ref, out_ref):
    rows = out_ref.shape[0]
    core = lax.rem(lax.axis_index("utt"), 2)
    out_ref[...] = cents_ref[pl.ds(pl.multiple_of(core * rows, rows), rows), :]


def cut(centroids):
    rows, width = centroids.shape
    return pl.pallas_call(
        cut_kernel,
        out_shape=jax.ShapeDtypeStruct((rows // 2, width), BF16),
        in_specs=[pl.BlockSpec(memory_space=VMEM)],
        out_specs=pl.BlockSpec(memory_space=VMEM),
        compiler_params=pltpu.CompilerParams(vmem_limit_bytes=2 << 20),
        cost_estimate=pl.CostEstimate(flops=1 << 20, bytes_accessed=1 << 20, transcendentals=0),
        name="cut",
    )(centroids)


def stage_kernel(feat_hbm, feat_ref, sem):
    copy = pltpu.make_async_copy(feat_hbm, feat_ref, sem)
    copy.start()
    copy.wait()


def staged(features):
    return pl.pallas_call(
        stage_kernel,
        out_shape=VMEM(features.shape, BF16),
        in_specs=[pl.BlockSpec(memory_space=pltpu.HBM)],
        out_specs=pl.BlockSpec(memory_space=VMEM),
        scratch_shapes=[pltpu.SemaphoreType.DMA(())],
        compiler_params=pltpu.CompilerParams(vmem_limit_bytes=1 << 20),
        cost_estimate=pl.CostEstimate(flops=1 << 30, bytes_accessed=5 << 20, transcendentals=0),
        name="staged",
    )(pltpu.with_memory_space_constraint(features, pltpu.HBM))


def square_kernel(feat_ref, sq_ref):
    frames, width = feat_ref.shape
    cell = 256
    eye = (
        lax.broadcasted_iota(jnp.int32, (cell, cell), 0) == lax.broadcasted_iota(jnp.int32, (cell, cell), 1)
    ).astype(BF16)
    for f in range(0, frames, cell):
        total = jnp.zeros((8, cell), F32)
        for k in range(0, width, cell):
            part = lax.dot_general(
                eye, feat_ref[f : f + cell, k : k + cell], (((1,), (1,)), ((), ())), preferred_element_type=F32
            )
            total = total + jnp.sum((part * part).reshape(cell // 8, 8, cell), axis=0)
        sq_ref[:, f : f + cell] = jnp.broadcast_to(jnp.sum(total, axis=0, keepdims=True), (8, cell))


def squares(features):
    frames, _ = features.shape
    return pl.pallas_call(
        square_kernel,
        out_shape=jax.ShapeDtypeStruct((8, frames), F32),
        in_specs=[pl.BlockSpec(memory_space=VMEM)],
        out_specs=pl.BlockSpec(memory_space=VMEM),
        compiler_params=pltpu.CompilerParams(vmem_limit_bytes=2 << 20),
        cost_estimate=pl.CostEstimate(flops=1 << 30, bytes_accessed=5 << 20, transcendentals=0),
        name="squares",
    )(features)


def score(cents, bases, own_ref, other_ref, least_in, index_in, least_ref, index_ref):
    rows = cents.shape[0] // len(bases)
    frames = own_ref.shape[0]
    tile = 256
    wide = cents.astype(F32)
    cent_sq = jnp.sum(wide * wide, axis=1, keepdims=True)
    scaled = cents * BF16(-2)
    sub = lax.broadcasted_iota(jnp.int32, (8, tile), 0)
    for side, feats in enumerate((own_ref, other_ref)):
        for f in range(0, frames, tile):
            at = slice(side * frames + f, side * frames + f + tile)
            dots = lax.dot_general(
                scaled, feats[f : f + tile], (((1,), (1,)), ((), ())), preferred_element_type=F32
            )
            least = index = None
            if least_in is not None:
                least, index = least_in[:, at], index_in[:, at]
            for block, base in enumerate(bases):
                low = where = None
                for r in range(0, rows, 8):
                    q = block * rows + r
                    value = dots[q : q + 8] + cent_sq[q : q + 8]
                    if low is None:
                        low, where = value, jnp.zeros((8, tile), jnp.int32)
                    else:
                        less = value < low
                        low = jnp.where(less, value, low)
                        where = jnp.where(less, r, where)
                where = where + (sub + base)
                if least is None:
                    least, index = low, where
                else:
                    better = (low < least) | ((low == least) & (where < index))
                    least = jnp.where(better, low, least)
                    index = jnp.where(better, where, index)
            least_ref[:, at] = least
            index_ref[:, at] = index


def pieces(value):
    high = value.astype(BF16)
    rest = value - high.astype(F32)
    middle = rest.astype(BF16)
    low = (rest - middle.astype(F32)).astype(BF16)
    return high, middle, low


def exact_dot(left, right):
    if left.dtype == F32:
        parts = [jnp.dot(p, right, preferred_element_type=F32) for p in pieces(left)]
    else:
        parts = [jnp.dot(left, p, preferred_element_type=F32) for p in pieces(right)]
    return (parts[0] + parts[1]) + parts[2]


def pack(least, index, square_ref, route_ref, other_route_ref, out_ref):
    frames = least.shape[1] // 2
    low = jnp.min(least, axis=0, keepdims=True)
    label = jnp.min(jnp.where(least == low, index, BIG), axis=0, keepdims=True).astype(F32)
    square = square_ref[0:1, :]
    sub = lax.broadcasted_iota(jnp.int32, (8, 128), 0)
    lane = lax.broadcasted_iota(jnp.int32, (8, 128), 1)
    mask = (lane // 16) == sub
    src = lax.broadcasted_iota(jnp.int32, (128, 128), 0)
    dst = lax.broadcasted_iota(jnp.int32, (128, 128), 1)

    def spread(row):
        groups = [
            jnp.where(mask, jnp.broadcast_to(row[:, i : i + 128], (8, 128)), 0.0) for i in range(0, frames, 128)
        ]
        return jnp.concatenate(groups, axis=0)

    def place(row, slot):
        pick = (dst == slot * 16 + lax.rem(src, 16)).astype(BF16)
        return exact_dot(spread(row), pick)

    own = place(low[:, :frames], 0) + place(label[:, :frames], 1) + place(square, 4)
    other = place(low[:, frames:], 2) + place(label[:, frames:], 3)
    to_own = (src == route_ref[0:1, :]).astype(BF16)
    to_other = (src == other_route_ref[0:1, :]).astype(BF16)
    out_ref[...] = exact_dot(to_own, own) + exact_dot(to_other, other)


def first_kernel(row, pair, own, other, least_ref, index_ref):
    rows = row.shape[0] // SIDE
    cents = jnp.concatenate([row[...], pair[...]], axis=0)
    score(cents, row_bases(0, rows) + pair_bases(True, rows), own, other, None, None, least_ref, index_ref)


def next_kernel(row, own, other, least_in, index_in, least_ref, index_ref):
    score(row[...], row_bases(1, row.shape[0] // SIDE), own, other, least_in, index_in, least_ref, index_ref)


def last_kernel(
    row, pair, own, other, least_in, index_in, square, route, other_route, out_ref, least_ref, index_ref
):
    rows = row.shape[0] // SIDE
    cents = jnp.concatenate([row[...], pair[...]], axis=0)
    bases = row_bases(-1, rows) + pair_bases(False, rows)
    score(cents, bases, own, other, least_in, index_in, least_ref, index_ref)
    pack(least_ref[...], index_ref[...], square, route, other_route, out_ref)


def scoring(kernel, args, out_shape, scratch=()):
    return pl.pallas_call(
        kernel,
        out_shape=out_shape,
        in_specs=[pl.BlockSpec(memory_space=VMEM)] * len(args),
        out_specs=jax.tree.map(lambda _: pl.BlockSpec(memory_space=VMEM), out_shape),
        scratch_shapes=list(scratch),
        compiler_params=pltpu.CompilerParams(vmem_limit_bytes=5 << 20),
        cost_estimate=pl.CostEstimate(flops=2 * 256 * 1280 * 4096, bytes_accessed=11 << 20, transcendentals=0),
    )(*args)


def merge_kernel(got_ref, label_ref, dist_ref, *, width):
    got = got_ref[...]
    turned = jnp.concatenate([got[r ^ 16 : (r ^ 16) + 16] for r in range(0, got.shape[0], 16)], axis=0)
    mine, theirs = got.T, turned.T
    low, label = mine[0:16], mine[16:32]
    other_low, other_label = theirs[32:48], theirs[48:64]
    better = (other_low < low) | ((other_low == low) & (other_label < label))
    label_ref[...] = jnp.where(better, other_label, label).astype(jnp.int32)
    dist_ref[...] = (mine[64:80] + jnp.where(better, other_low, low)) / width


def send(value, pairs):
    return lax.ppermute(value, AXES, pairs)


def labelled(features, centroids, route):
    frames, width = features.shape
    mine = cut(centroids)
    near = [mine] + [send(mine, along(o, 0)) for o in OFFSETS if o]
    pair = jnp.concatenate([send(mine, fetch(i)) for i in range(2)], axis=0)
    own = staged(features)
    other = send(features, core_swap())
    other_route = send(route, core_swap())
    square = squares(own)
    row = jnp.concatenate(near, axis=0)
    row_up = send(row, along(1, 1))
    row_down = send(row, along(-1, 1))
    other_pair = send(pair, plane_swap())
    state = (jax.ShapeDtypeStruct((8, 2 * frames), F32), jax.ShapeDtypeStruct((8, 2 * frames), jnp.int32))
    least, index = scoring(first_kernel, (row, pair, own, other), state)
    least, index = scoring(next_kernel, (row_up, own, other, least, index), state)
    packed = scoring(
        last_kernel,
        (row_down, other_pair, own, other, least, index, square, route, other_route),
        jax.ShapeDtypeStruct((128, 128), F32),
        scratch=[pltpu.VMEM((8, 2 * frames), F32), pltpu.VMEM((8, 2 * frames), jnp.int32)],
    )
    got = lax.all_to_all(packed, AXES, split_axis=0, concat_axis=0, tiled=True)
    label, dist = pl.pallas_call(
        functools.partial(merge_kernel, width=float(width)),
        out_shape=(jax.ShapeDtypeStruct((16, 128), jnp.int32), jax.ShapeDtypeStruct((16, 128), F32)),
        in_specs=[pl.BlockSpec(memory_space=VMEM)],
        out_specs=(pl.BlockSpec(memory_space=VMEM),) * 2,
        compiler_params=pltpu.CompilerParams(vmem_limit_bytes=2 << 20),
        name="merge",
    )(got)
    return label.T[None], dist.T[None]


def solution(mesh):
    placed = (P(AXES, None), P("clu", None), P(AXES, None))
    return jax.shard_map(
        labelled,
        mesh=mesh,
        in_specs=placed,
        out_specs=(P(AXES, None, None), P(AXES, None, None)),
        check_vma=False,
    )
```

```python
import functools

import jax
import jax.numpy as jnp
from jax import lax
from jax.experimental import pallas as pl
from jax.experimental.pallas import tpu as pltpu
from jax.sharding import PartitionSpec as P


AXES = ("utt", "clu")
SIDE = 4
VMEM = pltpu.VMEM
F32 = jnp.float32
BF16 = jnp.bfloat16
BIG = 1 << 20


def device(y, c, z, x):
    return (y * 2 + c) * 16 + (z % SIDE) * SIDE + x % SIDE


def everywhere(target):
    def at(y, c, near, far):
        return device(y, c, far, near) if c == 0 else device(y, c, near, far)

    return [
        (at(y, c, near, far), at(*target(y, c, near, far)))
        for y in range(4)
        for c in range(2)
        for near in range(SIDE)
        for far in range(SIDE)
    ]


def near_step(offset):
    return everywhere(lambda y, c, near, far: (y, c, near + offset, far))


def far_step(offset):
    return everywhere(lambda y, c, near, far: (y, c, near, far + offset))


def core_swap():
    return everywhere(lambda y, c, near, far: (y, 1 - c, far, near))


def place():
    core = lax.rem(lax.axis_index("utt"), 2)
    clu = lax.axis_index("clu")
    z, x = clu // SIDE, lax.rem(clu, SIDE)
    return core, jnp.where(core == 0, x, z), jnp.where(core == 0, z, x)


def half_bases(near_offsets, far_offset, rows):
    core, near, far = place()
    bases = []
    for offset in near_offsets:
        n = lax.rem(near + SIDE + offset, SIDE)
        f = lax.rem(far + SIDE + far_offset, SIDE)
        shard = jnp.where(core == 0, f * SIDE + n, n * SIDE + f)
        bases.append(shard * (2 * rows) + core * rows)
    return bases


FIRST = (0, -1)
SECOND = (1, -2)


def cut_kernel(cents_hbm, out_ref, sem):
    rows = out_ref.shape[0]
    core = lax.rem(lax.axis_index("utt"), 2)
    copy = pltpu.make_async_copy(cents_hbm.at[pl.ds(pl.multiple_of(core * rows, rows), rows)], out_ref, sem)
    copy.start()
    copy.wait()


def cut(centroids):
    rows, width = centroids.shape
    return pl.pallas_call(
        cut_kernel,
        out_shape=VMEM((rows // 2, width), BF16),
        in_specs=[pl.BlockSpec(memory_space=pltpu.HBM)],
        out_specs=pl.BlockSpec(memory_space=VMEM),
        scratch_shapes=[pltpu.SemaphoreType.DMA(())],
        compiler_params=pltpu.CompilerParams(vmem_limit_bytes=1 << 20),
        cost_estimate=pl.CostEstimate(flops=1 << 34, bytes_accessed=1 << 20, transcendentals=0),
        name="cut",
    )(pltpu.with_memory_space_constraint(centroids, pltpu.HBM))


def square_kernel(feat_ref, sq_ref):
    frames, width = feat_ref.shape
    cell = 256
    eye = (
        lax.broadcasted_iota(jnp.int32, (cell, cell), 0) == lax.broadcasted_iota(jnp.int32, (cell, cell), 1)
    ).astype(BF16)
    for f in range(0, frames, cell):
        total = jnp.zeros((8, cell), F32)
        for k in range(0, width, cell):
            part = lax.dot_general(
                eye, feat_ref[f : f + cell, k : k + cell], (((1,), (1,)), ((), ())), preferred_element_type=F32
            )
            total = total + jnp.sum((part * part).reshape(cell // 8, 8, cell), axis=0)
        sq_ref[:, f : f + cell] = jnp.broadcast_to(jnp.sum(total, axis=0, keepdims=True), (8, cell))


def squares(features):
    frames, _ = features.shape
    return pl.pallas_call(
        square_kernel,
        out_shape=jax.ShapeDtypeStruct((8, frames), F32),
        in_specs=[pl.BlockSpec(memory_space=VMEM)],
        out_specs=pl.BlockSpec(memory_space=VMEM),
        compiler_params=pltpu.CompilerParams(vmem_limit_bytes=2 << 20),
        cost_estimate=pl.CostEstimate(flops=1 << 30, bytes_accessed=5 << 20, transcendentals=0),
        name="squares",
    )(features)


def score(cents, bases, own_ref, other_ref, least_in, index_in, least_ref, index_ref):
    rows = cents.shape[0] // len(bases)
    frames = own_ref.shape[0]
    tile = 256
    wide = cents.astype(F32)
    cent_sq = jnp.sum(wide * wide, axis=1, keepdims=True)
    scaled = cents * BF16(-2)
    sub = lax.broadcasted_iota(jnp.int32, (8, tile), 0)
    for side, feats in enumerate((own_ref, other_ref)):
        for f in range(0, frames, tile):
            at = slice(side * frames + f, side * frames + f + tile)
            dots = lax.dot_general(
                scaled, feats[f : f + tile], (((1,), (1,)), ((), ())), preferred_element_type=F32
            )
            least = index = None
            if least_in is not None:
                least, index = least_in[:, at], index_in[:, at]
            for block, base in enumerate(bases):
                low = where = None
                for r in range(0, rows, 8):
                    q = block * rows + r
                    value = dots[q : q + 8] + cent_sq[q : q + 8]
                    if low is None:
                        low, where = value, jnp.zeros((8, tile), jnp.int32)
                    else:
                        less = value < low
                        low = jnp.where(less, value, low)
                        where = jnp.where(less, r, where)
                where = where + (sub + base)
                if least is None:
                    least, index = low, where
                else:
                    better = (low < least) | ((low == least) & (where < index))
                    least = jnp.where(better, low, least)
                    index = jnp.where(better, where, index)
            least_ref[:, at] = least
            index_ref[:, at] = index


def pieces(value):
    high = value.astype(BF16)
    rest = value - high.astype(F32)
    middle = rest.astype(BF16)
    low = (rest - middle.astype(F32)).astype(BF16)
    return high, middle, low


def exact_dot(left, right):
    if left.dtype == F32:
        parts = [jnp.dot(p, right, preferred_element_type=F32) for p in pieces(left)]
    else:
        parts = [jnp.dot(left, p, preferred_element_type=F32) for p in pieces(right)]
    return (parts[0] + parts[1]) + parts[2]


def pack(least, index, square_ref, route_ref, other_route_ref, out_ref):
    frames = least.shape[1] // 2
    low = jnp.min(least, axis=0, keepdims=True)
    label = jnp.min(jnp.where(least == low, index, BIG), axis=0, keepdims=True).astype(F32)
    square = square_ref[0:1, :]
    sub = lax.broadcasted_iota(jnp.int32, (8, 128), 0)
    lane = lax.broadcasted_iota(jnp.int32, (8, 128), 1)
    mask = (lane // 16) == sub
    src = lax.broadcasted_iota(jnp.int32, (128, 128), 0)
    dst = lax.broadcasted_iota(jnp.int32, (128, 128), 1)

    def spread(row):
        groups = [
            jnp.where(mask, jnp.broadcast_to(row[:, i : i + 128], (8, 128)), 0.0) for i in range(0, frames, 128)
        ]
        return jnp.concatenate(groups, axis=0)

    def place(row, slot):
        pick = (dst == slot * 16 + lax.rem(src, 16)).astype(BF16)
        return exact_dot(spread(row), pick)

    own = place(low[:, :frames], 0) + place(label[:, :frames], 1) + place(square, 4)
    other = place(low[:, frames:], 2) + place(label[:, frames:], 3)
    to_own = (src == route_ref[0:1, :]).astype(BF16)
    to_other = (src == other_route_ref[0:1, :]).astype(BF16)
    out_ref[...] = exact_dot(to_own, own) + exact_dot(to_other, other)


def halves(first, first_from, second, second_from):
    rows = first.shape[0] // 2
    bases = half_bases(FIRST, first_from, rows) + half_bases(SECOND, second_from, rows)
    return jnp.concatenate([first[...], second[...]], axis=0), bases


def first_kernel(first, second, own, other, least_ref, index_ref):
    cents, bases = halves(first, 0, second, 0)
    score(cents, bases, own, other, None, None, least_ref, index_ref)


def next_kernel(first_from, second_from, first, second, own, other, least_in, index_in, least_ref, index_ref):
    cents, bases = halves(first, first_from, second, second_from)
    score(cents, bases, own, other, least_in, index_in, least_ref, index_ref)


def last_kernel(
    first, second, own, other, least_in, index_in, square, route, other_route, out_ref, least_ref, index_ref
):
    cents, bases = halves(first, 2, second, 2)
    score(cents, bases, own, other, least_in, index_in, least_ref, index_ref)
    pack(least_ref[...], index_ref[...], square, route, other_route, out_ref)


def scoring(kernel, args, out_shape, scratch=()):
    return pl.pallas_call(
        kernel,
        out_shape=out_shape,
        in_specs=[pl.BlockSpec(memory_space=VMEM)] * len(args),
        out_specs=jax.tree.map(lambda _: pl.BlockSpec(memory_space=VMEM), out_shape),
        scratch_shapes=list(scratch),
        compiler_params=pltpu.CompilerParams(vmem_limit_bytes=5 << 20),
        cost_estimate=pl.CostEstimate(flops=2 * 256 * 1280 * 4096, bytes_accessed=11 << 20, transcendentals=0),
    )(*args)


def merge_kernel(got_ref, label_ref, dist_ref, *, width):
    got = got_ref[...]
    turned = jnp.concatenate([got[r ^ 16 : (r ^ 16) + 16] for r in range(0, got.shape[0], 16)], axis=0)
    mine, theirs = got.T, turned.T
    low, label = mine[0:16], mine[16:32]
    other_low, other_label = theirs[32:48], theirs[48:64]
    better = (other_low < low) | ((other_low == low) & (other_label < label))
    label_ref[...] = jnp.where(better, other_label, label).astype(jnp.int32)
    dist_ref[...] = (mine[64:80] + jnp.where(better, other_low, low)) / width


def send(value, pairs):
    return lax.ppermute(value, AXES, pairs)


def labelled(features, centroids, route):
    frames, width = features.shape
    other = send(features, core_swap())
    other_route = send(route, core_swap())
    mine = cut(centroids)
    near1 = send(mine, near_step(1))
    near2 = send(mine, near_step(-1))
    near3 = send(mine, near_step(2))
    first = jnp.concatenate([mine, near1], axis=0)
    second = jnp.concatenate([near2, near3], axis=0)
    up_first = send(first, far_step(1))
    down_second = send(second, far_step(-1))
    up_second = send(second, far_step(1))
    down_first = send(first, far_step(-1))
    over_first = send(up_first, far_step(1))
    over_second = send(down_second, far_step(-1))
    own = pltpu.with_memory_space_constraint(features, VMEM)
    square = squares(own)
    state = (jax.ShapeDtypeStruct((8, 2 * frames), F32), jax.ShapeDtypeStruct((8, 2 * frames), jnp.int32))
    least, index = scoring(first_kernel, (first, second, own, other), state)
    least, index = scoring(
        functools.partial(next_kernel, -1, 1), (up_first, down_second, own, other, least, index), state
    )
    least, index = scoring(
        functools.partial(next_kernel, 1, -1), (down_first, up_second, own, other, least, index), state
    )
    packed = scoring(
        last_kernel,
        (over_first, over_second, own, other, least, index, square, route, other_route),
        jax.ShapeDtypeStruct((128, 128), F32),
        scratch=[pltpu.VMEM((8, 2 * frames), F32), pltpu.VMEM((8, 2 * frames), jnp.int32)],
    )
    got = lax.all_to_all(packed, AXES, split_axis=0, concat_axis=0, tiled=True)
    label, dist = pl.pallas_call(
        functools.partial(merge_kernel, width=float(width)),
        out_shape=(jax.ShapeDtypeStruct((16, 128), jnp.int32), jax.ShapeDtypeStruct((16, 128), F32)),
        in_specs=[pl.BlockSpec(memory_space=VMEM)],
        out_specs=(pl.BlockSpec(memory_space=VMEM),) * 2,
        compiler_params=pltpu.CompilerParams(vmem_limit_bytes=2 << 20),
        name="merge",
    )(got)
    return label.T[None], dist.T[None]


def solution(mesh):
    placed = (P(AXES, None), P("clu", None), P(AXES, None))
    return jax.shard_map(
        labelled,
        mesh=mesh,
        in_specs=placed,
        out_specs=(P(AXES, None, None), P(AXES, None, None)),
        check_vma=False,
    )
```

```python
import functools

import jax
import jax.numpy as jnp
from jax import lax
from jax.experimental import pallas as pl
from jax.experimental.pallas import tpu as pltpu
from jax.sharding import PartitionSpec as P


AXES = ("utt", "clu")
SIDE = 4
VMEM = pltpu.VMEM
F32 = jnp.float32
BF16 = jnp.bfloat16
BIG = 1 << 20


def device(y, c, z, x):
    return (y * 2 + c) * 16 + (z % SIDE) * SIDE + x % SIDE


def everywhere(target):
    def at(y, c, near, far):
        return device(y, c, far, near) if c == 0 else device(y, c, near, far)

    return [
        (at(y, c, near, far), at(*target(y, c, near, far)))
        for y in range(4)
        for c in range(2)
        for near in range(SIDE)
        for far in range(SIDE)
    ]


def near_step(offset):
    return everywhere(lambda y, c, near, far: (y, c, near + offset, far))


def far_step(offset):
    return everywhere(lambda y, c, near, far: (y, c, near, far + offset))


def core_swap():
    return everywhere(lambda y, c, near, far: (y, 1 - c, far, near))


def place():
    core = lax.rem(lax.axis_index("utt"), 2)
    clu = lax.axis_index("clu")
    z, x = clu // SIDE, lax.rem(clu, SIDE)
    return core, jnp.where(core == 0, x, z), jnp.where(core == 0, z, x)


def half_bases(near_offsets, far_offset, rows):
    core, near, far = place()
    bases = []
    for offset in near_offsets:
        n = lax.rem(near + SIDE + offset, SIDE)
        f = lax.rem(far + SIDE + far_offset, SIDE)
        shard = jnp.where(core == 0, f * SIDE + n, n * SIDE + f)
        bases.append(shard * (2 * rows) + core * rows)
    return bases


FIRST = (0, -1)
SECOND = (1, -2)


def cut_kernel(cents_hbm, out_ref, sem):
    rows = out_ref.shape[0]
    core = lax.rem(lax.axis_index("utt"), 2)
    copy = pltpu.make_async_copy(cents_hbm.at[pl.ds(pl.multiple_of(core * rows, rows), rows)], out_ref, sem)
    copy.start()
    copy.wait()


def cut(centroids):
    rows, width = centroids.shape
    return pl.pallas_call(
        cut_kernel,
        out_shape=VMEM((rows // 2, width), BF16),
        in_specs=[pl.BlockSpec(memory_space=pltpu.HBM)],
        out_specs=pl.BlockSpec(memory_space=VMEM),
        scratch_shapes=[pltpu.SemaphoreType.DMA(())],
        compiler_params=pltpu.CompilerParams(vmem_limit_bytes=1 << 20),
        cost_estimate=pl.CostEstimate(flops=1 << 34, bytes_accessed=1 << 20, transcendentals=0),
        name="cut",
    )(pltpu.with_memory_space_constraint(centroids, pltpu.HBM))


def square_kernel(feat_ref, route_ref, out_ref, sq_ref):
    frames, width = feat_ref.shape
    cell = 256
    eye = (
        lax.broadcasted_iota(jnp.int32, (cell, cell), 0) == lax.broadcasted_iota(jnp.int32, (cell, cell), 1)
    ).astype(BF16)
    for f in range(0, frames, cell):
        total = jnp.zeros((8, cell), F32)
        for k in range(0, width, cell):
            part = lax.dot_general(
                eye, feat_ref[f : f + cell, k : k + cell], (((1,), (1,)), ((), ())), preferred_element_type=F32
            )
            total = total + jnp.sum((part * part).reshape(cell // 8, 8, cell), axis=0)
        sq_ref[:, f : f + cell] = jnp.broadcast_to(jnp.sum(total, axis=0, keepdims=True), (8, cell))
    out_ref[...] = exact_dot(by_route(route_ref), put(sq_ref[0:1, :], 4))


def score(cents, bases, own_ref, other_ref, least_in, index_in, least_ref, index_ref):
    rows = cents.shape[0] // len(bases)
    frames = own_ref.shape[0]
    tile = 256
    wide = cents.astype(F32)
    cent_sq = jnp.sum(wide * wide, axis=1, keepdims=True)
    scaled = cents * BF16(-2)
    sub = lax.broadcasted_iota(jnp.int32, (8, tile), 0)
    for side, feats in enumerate((own_ref, other_ref)):
        for f in range(0, frames, tile):
            at = slice(side * frames + f, side * frames + f + tile)
            dots = lax.dot_general(
                scaled, feats[f : f + tile], (((1,), (1,)), ((), ())), preferred_element_type=F32
            )
            least = index = None
            if least_in is not None:
                least, index = least_in[:, at], index_in[:, at]
            for block, base in enumerate(bases):
                low = where = None
                for r in range(0, rows, 8):
                    q = block * rows + r
                    value = dots[q : q + 8] + cent_sq[q : q + 8]
                    if low is None:
                        low, where = value, jnp.zeros((8, tile), jnp.int32)
                    else:
                        less = value < low
                        low = jnp.where(less, value, low)
                        where = jnp.where(less, r, where)
                where = where + (sub + base)
                if least is None:
                    least, index = low, where
                else:
                    better = (low < least) | ((low == least) & (where < index))
                    least = jnp.where(better, low, least)
                    index = jnp.where(better, where, index)
            least_ref[:, at] = least
            index_ref[:, at] = index


def pieces(value, count):
    parts = []
    for _ in range(count):
        part = value.astype(BF16)
        parts.append(part)
        value = value - part.astype(F32)
    return parts


def exact_dot(left, right, count=3):
    if left.dtype == F32:
        parts = [jnp.dot(p, right, preferred_element_type=F32) for p in pieces(left, count)]
    else:
        parts = [jnp.dot(left, p, preferred_element_type=F32) for p in pieces(right, count)]
    return sum(parts[1:], parts[0])


def put(row, slot, count=3):
    sub = lax.broadcasted_iota(jnp.int32, (8, 128), 0)
    lane = lax.broadcasted_iota(jnp.int32, (8, 128), 1)
    mask = (lane // 16) == sub
    src = lax.broadcasted_iota(jnp.int32, (128, 128), 0)
    dst = lax.broadcasted_iota(jnp.int32, (128, 128), 1)
    groups = [
        jnp.where(mask, jnp.broadcast_to(row[:, i : i + 128], (8, 128)), 0.0) for i in range(0, row.shape[1], 128)
    ]
    pick = (dst == slot * 16 + lax.rem(src, 16)).astype(BF16)
    return exact_dot(jnp.concatenate(groups, axis=0), pick, count)


def by_route(route_ref):
    trainer = lax.broadcasted_iota(jnp.int32, (128, 128), 0)
    return (trainer == route_ref[0:1, :]).astype(BF16)


def pack(least, index, square_ref, route_ref, other_route_ref, out_ref):
    frames = least.shape[1] // 2
    low = jnp.min(least, axis=0, keepdims=True)
    label = jnp.min(jnp.where(least == low, index, BIG), axis=0, keepdims=True).astype(F32)
    own = put(low[:, :frames], 0) + put(label[:, :frames], 1, 2)
    other = put(low[:, frames:], 2) + put(label[:, frames:], 3, 2)
    out_ref[...] = (
        exact_dot(by_route(route_ref), own) + exact_dot(by_route(other_route_ref), other) + square_ref[...]
    )


def squares(features, route):
    frames = features.shape[0]
    return pl.pallas_call(
        square_kernel,
        out_shape=jax.ShapeDtypeStruct((128, 128), F32),
        in_specs=[pl.BlockSpec(memory_space=VMEM)] * 2,
        out_specs=pl.BlockSpec(memory_space=VMEM),
        scratch_shapes=[pltpu.VMEM((8, frames), F32)],
        compiler_params=pltpu.CompilerParams(vmem_limit_bytes=2 << 20),
        cost_estimate=pl.CostEstimate(flops=1 << 30, bytes_accessed=5 << 20, transcendentals=0),
        name="squares",
    )(features, route)


def halves(first, first_from, second, second_from):
    rows = first.shape[0] // 2
    bases = half_bases(FIRST, first_from, rows) + half_bases(SECOND, second_from, rows)
    return jnp.concatenate([first[...], second[...]], axis=0), bases


def first_kernel(first, second, own, other, least_ref, index_ref):
    cents, bases = halves(first, 0, second, 0)
    score(cents, bases, own, other, None, None, least_ref, index_ref)


def next_kernel(first_from, second_from, first, second, own, other, least_in, index_in, least_ref, index_ref):
    cents, bases = halves(first, first_from, second, second_from)
    score(cents, bases, own, other, least_in, index_in, least_ref, index_ref)


def last_kernel(
    first, second, own, other, least_in, index_in, square, route, other_route, out_ref, least_ref, index_ref
):
    cents, bases = halves(first, 2, second, 2)
    score(cents, bases, own, other, least_in, index_in, least_ref, index_ref)
    pack(least_ref[...], index_ref[...], square, route, other_route, out_ref)


def scoring(kernel, args, out_shape, scratch=()):
    return pl.pallas_call(
        kernel,
        out_shape=out_shape,
        in_specs=[pl.BlockSpec(memory_space=VMEM)] * len(args),
        out_specs=jax.tree.map(lambda _: pl.BlockSpec(memory_space=VMEM), out_shape),
        scratch_shapes=list(scratch),
        compiler_params=pltpu.CompilerParams(vmem_limit_bytes=5 << 20),
        cost_estimate=pl.CostEstimate(flops=2 * 256 * 1280 * 4096, bytes_accessed=11 << 20, transcendentals=0),
    )(*args)


def merge_kernel(got_ref, label_ref, dist_ref, *, width):
    got = got_ref[...]
    turned = jnp.concatenate([got[r ^ 16 : (r ^ 16) + 16] for r in range(0, got.shape[0], 16)], axis=0)
    mine, theirs = got.T, turned.T
    low, label = mine[0:16], mine[16:32]
    other_low, other_label = theirs[32:48], theirs[48:64]
    better = (other_low < low) | ((other_low == low) & (other_label < label))
    label_ref[...] = jnp.where(better, other_label, label).astype(jnp.int32)
    dist_ref[...] = (mine[64:80] + jnp.where(better, other_low, low)) / width


def send(value, pairs):
    return lax.ppermute(value, AXES, pairs)


def labelled(features, centroids, route):
    frames, width = features.shape
    other = send(features, core_swap())
    other_route = send(route, core_swap())
    mine = cut(centroids)
    near1 = send(mine, near_step(1))
    near2 = send(mine, near_step(-1))
    near3 = send(mine, near_step(2))
    first = jnp.concatenate([mine, near1], axis=0)
    second = jnp.concatenate([near2, near3], axis=0)
    up_first = send(first, far_step(1))
    down_second = send(second, far_step(-1))
    up_second = send(second, far_step(1))
    down_first = send(first, far_step(-1))
    over_first = send(up_first, far_step(1))
    over_second = send(down_second, far_step(-1))
    own = pltpu.with_memory_space_constraint(features, VMEM)
    square = squares(own, route)
    state = (jax.ShapeDtypeStruct((8, 2 * frames), F32), jax.ShapeDtypeStruct((8, 2 * frames), jnp.int32))
    least, index = scoring(first_kernel, (first, second, own, other), state)
    least, index = scoring(
        functools.partial(next_kernel, -1, 1), (up_first, down_second, own, other, least, index), state
    )
    least, index = scoring(
        functools.partial(next_kernel, 1, -1), (down_first, up_second, own, other, least, index), state
    )
    packed = scoring(
        last_kernel,
        (over_first, over_second, own, other, least, index, square, route, other_route),
        jax.ShapeDtypeStruct((128, 128), F32),
        scratch=[pltpu.VMEM((8, 2 * frames), F32), pltpu.VMEM((8, 2 * frames), jnp.int32)],
    )
    got = lax.all_to_all(packed, AXES, split_axis=0, concat_axis=0, tiled=True)
    label, dist = pl.pallas_call(
        functools.partial(merge_kernel, width=float(width)),
        out_shape=(jax.ShapeDtypeStruct((16, 128), jnp.int32), jax.ShapeDtypeStruct((16, 128), F32)),
        in_specs=[pl.BlockSpec(memory_space=VMEM)],
        out_specs=(pl.BlockSpec(memory_space=VMEM),) * 2,
        compiler_params=pltpu.CompilerParams(vmem_limit_bytes=2 << 20),
        name="merge",
    )(got)
    return label.T[None], dist.T[None]


def solution(mesh):
    placed = (P(AXES, None), P("clu", None), P(AXES, None))
    return jax.shard_map(
        labelled,
        mesh=mesh,
        in_specs=placed,
        out_specs=(P(AXES, None, None), P(AXES, None, None)),
        check_vma=False,
    )
```
